32 devices in a mesh: gx: 4 (over y, x), gy: 4 (over z), gz: 2 (over core).
Axes of the slice: x: 2, y: 2, z: 4, core: 2. Of those that a mesh axis runs over, the one named last changes fastest.
Arguments:
- right_side: float32 [3, 32, 128, 256], P(None, 'gx', 'gy', 'gz'), may hold values from -6 to 6
- mass_coef: float32 [3, 32, 128, 256], P(None, 'gx', 'gy', 'gz'), may hold values from 0.3 to 3
- curl_coef: float32 [3, 32, 128, 256], P(None, 'gx', 'gy', 'gz'), may hold values from 0.5 to 5
Outputs:
- solution: float32 [3, 32, 128, 256], P(None, 'gx', 'gy', 'gz')
- residual: float32 [3, 32, 128, 256], P(None, 'gx', 'gy', 'gz')
The draws below stay inside these ranges and needn't reach their ends.
All inputs are finite; a program needn't handle non-finite values.
Results may differ from the reference program's by a relative error of at most 0.0003.
Values sent between devices are 32-bit elements; how exact they have to be, the bound alone decides.
A program may use at most 64 MiB of HBM per device.

```python
import math
import jax
import jax.numpy as jnp
from jax import lax

ITERS = 4
NX = 32
NY = 128
NZ = 256


def block_levels(own_key, dims, split, smallest, largest):
    gain = 1.0
    for axis_at, parts in split:
        draws = jax.random.uniform(jax.random.fold_in(jax.random.fold_in(own_key, 6), axis_at), (parts,), jnp.float32, smallest / len(split), largest / len(split))
        gain = gain * jnp.repeat(jnp.exp(draws), dims[axis_at] // parts).reshape((-1,) + (1,) * (len(dims) - 1 - axis_at))
    return gain


def bell_draw(own_key, extent, spread, limit, split=(), held_as=jnp.bfloat16):
    loudness = block_levels(own_key, extent, split, -0.22, 0.18) if split else 1.0
    result = jax.random.normal(own_key, extent, jnp.float32) * spread * loudness
    return jnp.minimum(jnp.maximum(result, -limit), limit).astype(held_as)


def setup_inputs(seed: int = 0) -> dict:
    keys = jax.random.split(jax.random.key(seed), 4)
    return {
        "right_side": bell_draw(keys[0], (3, NX, NY, NZ), 1.0, 6.0, ((1, 4), (2, 4), (3, 2)), jnp.float32),
        "mass_coef": jnp.clip(jnp.exp(math.log(3.0) - 2.3025851 * jax.random.uniform(keys[1], (3, NX, NY, NZ), jnp.float32) ** block_levels(keys[1], (3, NX, NY, NZ), ((1, 4), (2, 4), (3, 2)), -0.2, 0.2)), 0.3, 3.0),
        "curl_coef": jnp.clip(jnp.exp(math.log(5.0) - 2.3025851 * jax.random.uniform(keys[2], (3, NX, NY, NZ), jnp.float32) ** block_levels(keys[2], (3, NX, NY, NZ), ((1, 4), (2, 4), (3, 2)), -0.2, 0.2)), 0.5, 5.0),
    }


def region(values, start, size):
    return lax.slice(values, tuple(start), tuple(s + n for s, n in zip(start, size)))


def shifted(values, size, base, dim, delta):
    start = [base, base, base]
    if dim >= 0:
        start[dim] = start[dim] + delta
    return region(values, start, size)


def apply_curl(padded, sigma_pad, mu_pad):
    inner = tuple(n - 2 for n in padded.shape[1:])
    faces = tuple(n - 1 for n in padded.shape[1:])
    along_x, along_y, along_z = padded[0], padded[1], padded[2]

    def face_at(values, dim):
        return shifted(values, faces, 0, dim, 1)

    def out_at(values, dim):
        return shifted(values, inner, 1, dim, -1)

    flux_x = (face_at(along_z, 1) - face_at(along_z, -1)) - (face_at(along_y, 2) - face_at(along_y, -1))
    flux_y = (face_at(along_x, 2) - face_at(along_x, -1)) - (face_at(along_z, 0) - face_at(along_z, -1))
    flux_z = (face_at(along_y, 0) - face_at(along_y, -1)) - (face_at(along_x, 1) - face_at(along_x, -1))
    weighted_x = face_at(mu_pad[0], -1) * flux_x
    weighted_y = face_at(mu_pad[1], -1) * flux_y
    weighted_z = face_at(mu_pad[2], -1) * flux_z
    result_x = (out_at(weighted_y, 2) - out_at(weighted_y, -1)) - (out_at(weighted_z, 1) - out_at(weighted_z, -1)) + out_at(sigma_pad[0], -1) * out_at(along_x, -1)
    result_y = (out_at(weighted_z, 0) - out_at(weighted_z, -1)) - (out_at(weighted_x, 2) - out_at(weighted_x, -1)) + out_at(sigma_pad[1], -1) * out_at(along_y, -1)
    result_z = (out_at(weighted_x, 1) - out_at(weighted_x, -1)) - (out_at(weighted_y, 0) - out_at(weighted_y, -1)) + out_at(sigma_pad[2], -1) * out_at(along_z, -1)
    return jnp.stack([result_x, result_y, result_z])


def edge_inverse(sigma_pad, mu_pad):
    inner = tuple(n - 2 for n in sigma_pad.shape[1:])

    def out_at(values, dim):
        return shifted(values, inner, 1, dim, -1)

    diag_x = out_at(sigma_pad[0], -1) + out_at(mu_pad[1], -1) + out_at(mu_pad[1], 2) + out_at(mu_pad[2], -1) + out_at(mu_pad[2], 1)
    diag_y = out_at(sigma_pad[1], -1) + out_at(mu_pad[2], -1) + out_at(mu_pad[2], 0) + out_at(mu_pad[0], -1) + out_at(mu_pad[0], 2)
    diag_z = out_at(sigma_pad[2], -1) + out_at(mu_pad[0], -1) + out_at(mu_pad[0], 1) + out_at(mu_pad[1], -1) + out_at(mu_pad[1], 0)
    return 1.0 / jnp.stack([diag_x, diag_y, diag_z])


def node_inverse(sigma_pad):
    nodes = tuple(n - 1 for n in sigma_pad.shape[1:])
    total = jnp.zeros(nodes, jnp.float32)
    for comp in range(3):
        total = total + shifted(sigma_pad[comp], nodes, 1, -1, 0) + shifted(sigma_pad[comp], nodes, 1, comp, -1)
    return 1.0 / total


def apply_aux(padded, edge_inv, node_inv):
    nodes = tuple(n - 1 for n in padded.shape[1:])
    inner = tuple(n - 2 for n in padded.shape[1:])
    nodal = jnp.zeros(nodes, jnp.float32)
    for comp in range(3):
        nodal = nodal + shifted(padded[comp], nodes, 1, comp, -1) - shifted(padded[comp], nodes, 1, -1, 0)
    potential = nodal * node_inv
    gradient = jnp.stack([shifted(potential, inner, 0, comp, 1) - shifted(potential, inner, 0, -1, 0) for comp in range(3)])
    return padded[:, 1:-1, 1:-1, 1:-1] * edge_inv + gradient


def wrap_pad(values):
    return jnp.pad(values, ((0, 0), (1, 1), (1, 1), (1, 1)), mode="wrap")


def reference(right_side, mass_coef, curl_coef):
    sigma_pad = wrap_pad(mass_coef)
    mu_pad = wrap_pad(curl_coef)
    edge_inv = edge_inverse(sigma_pad, mu_pad)
    node_inv = node_inverse(sigma_pad)

    def pair(values):
        precond = apply_aux(wrap_pad(values), edge_inv, node_inv)
        return precond, apply_curl(wrap_pad(precond), sigma_pad, mu_pad)

    solution = jnp.zeros_like(right_side)
    residual = right_side
    precond_res, image_res = pair(residual)
    direction = jnp.zeros_like(right_side)
    dir_image = jnp.zeros_like(right_side)
    dir_precond = jnp.zeros_like(right_side)
    dir_double = jnp.zeros_like(right_side)
    gamma_old = jnp.float32(1.0)
    alpha_old = jnp.float32(1.0)
    for iteration in range(ITERS):
        gamma_now = jnp.sum(residual * precond_res)
        delta_now = jnp.sum(image_res * precond_res)
        precond_img, image_img = pair(image_res)
        if iteration == 0:
            beta_now = jnp.float32(0.0)
            alpha_now = gamma_now / delta_now
        else:
            beta_now = gamma_now / gamma_old
            alpha_now = gamma_now / (delta_now - beta_now * gamma_now / alpha_old)
        dir_double = image_img + beta_now * dir_double
        dir_precond = precond_img + beta_now * dir_precond
        dir_image = image_res + beta_now * dir_image
        direction = precond_res + beta_now * direction
        solution = solution + alpha_now * direction
        residual = residual - alpha_now * dir_image
        precond_res = precond_res - alpha_now * dir_precond
        image_res = image_res - alpha_now * dir_double
        gamma_old = gamma_now
        alpha_old = alpha_now
    return solution, residual
```

```python
import functools

import jax
import jax.numpy as jnp
from jax import lax
from jax.experimental import pallas as pl
from jax.experimental.pallas import tpu as pltpu
from jax.sharding import PartitionSpec as P

ITERS = 4
SHIFT = 1.5
PAD = 8
MESH = pl.DeviceIdType.MESH


def kernel(sizes, r_ref, m_ref, c_ref, x_out, res_out, V, E, C, ZV, ZE, CZ, MX, MZ, YS, YR, LS, LR,
           PH, S, G, BK, VL, RED, send, recv, csend, crecv, rsend, rrecv):
    nx, ny, nz = sizes
    total = nx * ny * nz
    _, X, Y, Z = r_ref.shape
    ix, iy, iz = (lax.axis_index(a) for a in ("gx", "gy", "gz"))
    rank = (ix * ny + iy) * nz + iz
    sides = ZV.shape[1]
    north = sides - 1
    Yh = Y + PAD
    YE = Y + 2 * PAD
    loc = pl.ds(PAD, Y)
    inx = pl.ds(1, X)

    def dev(dx, dy, dz):
        return (lax.rem(ix + dx + nx, nx), lax.rem(iy + dy + ny, ny), lax.rem(iz + dz + nz, nz))

    def ranked(i):
        return (i // (ny * nz), lax.rem(i // nz, ny), lax.rem(i, nz))

    barrier = pltpu.get_barrier_semaphore()

    @pl.loop(1, total)
    def _(o):
        pl.semaphore_signal(
            barrier, inc=1, device_id=ranked(lax.rem(rank + o, total)), device_id_type=MESH
        )

    lane = lax.broadcasted_iota(jnp.int32, (Y, Z), 1)
    row = lax.broadcasted_iota(jnp.int32, (Y, Z), 0)
    lane_h = lax.broadcasted_iota(jnp.int32, (Yh, Z), 1)
    pending = []

    def remote(src, dst, ss, rs, to):
        copy = pltpu.make_async_remote_copy(
            src_ref=src, dst_ref=dst, send_sem=ss, recv_sem=rs, device_id=to, device_id_type=MESH
        )
        copy.start()
        pending.append(copy)
        return copy

    def up_z(own, other):
        ln = lane if own.shape[0] == Y else lane_h
        return pltpu.roll(jnp.where(ln == 0, other, own), Z - 1, 1)

    def dn_z(own, other):
        ln = lane if own.shape[0] == Y else lane_h
        return pltpu.roll(jnp.where(ln == Z - 1, other, own), 1, 1)

    def to_row(col):
        n = col.shape[0]
        wide = jnp.broadcast_to(col, (n, Z))
        return jnp.sum(jnp.where(row[:n] == lane[:n], wide, 0.0), axis=0, keepdims=True)

    def to_col(line, n):
        wide = jnp.broadcast_to(line, (n, Z))
        col = jnp.sum(jnp.where(row[:n] == lane[:n], wide, 0.0), axis=1, keepdims=True)
        return jnp.broadcast_to(col, (n, Z))

    def stage(p, F, down_y):
        for c in range(3):
            YS[p, 0, c] = F[c, 1 : X + 1, PAD + Y - 1, :]
            YS[p, 1, c] = F[down_y[c], 1 : X + 1, PAD, :]
        LS[p, 0] = F[0, X, PAD : PAD + 1, :]
        LS[p, 1] = F[1, 1, PAD + Y - 1 : PAD + Y, :]
        LS[p, 2] = to_row(F[0, X, loc, :][:, 0:1])
        LS[p, 3] = to_row(F[2, 1, loc, :][:, Z - 1 : Z])
        LS[p, 4] = to_row(YS[p, 0, 1][:, 0:1])
        LS[p, 5] = to_row(YS[p, 1, 2][:, Z - 1 : Z])

    line_to = ((1, -1, 0), (-1, 1, 0), (1, 0, -1), (-1, 0, 1), (0, 1, -1), (0, -1, 1))

    def launch(p, F, ZB, down_x):
        def sem(n):
            return send.at[p, n], recv.at[p, n]

        out = [
            remote(F.at[pl.ds(0, 3), X, loc], F.at[pl.ds(0, 3), 0, loc], *sem(0), dev(1, 0, 0)),
            remote(
                F.at[pl.ds(down_x, 3), 1, loc], F.at[pl.ds(down_x, 3), X + 1, loc], *sem(1),
                dev(-1, 0, 0),
            ),
            remote(YS.at[p, 0], YR.at[p, 0], *sem(2), dev(0, 1, 0)),
            remote(YS.at[p, 1], YR.at[p, 1], *sem(3), dev(0, -1, 0)),
        ]
        for n in range(6):
            out.append(remote(LS.at[p, n], LR.at[p, n], *sem(4 + n), dev(*line_to[n])))
        for n in range(sides):
            out.append(
                remote(
                    F.at[:, inx, loc], ZB.at[n, :, inx, loc], *sem(10 + n),
                    dev(0, 0, 1 if n == 0 else -1),
                )
            )
        return out

    def land(p, F, ZB, down_y, copies):
        for copy in copies:
            copy.wait_recv()
        for c in range(3):
            F[c, 1 : X + 1, PAD - 1, :] = YR[p, 0, c]
            F[down_y[c], 1 : X + 1, PAD + Y, :] = YR[p, 1, c]
        F[0, 0, PAD + Y : PAD + Y + 1, :] = LR[p, 0]
        F[1, X + 1, PAD - 1 : PAD, :] = LR[p, 1]
        ZB[north, 0, 0, loc, :] = to_col(LR[p, 2], Y)
        ZB[0, 2, X + 1, loc, :] = to_col(LR[p, 3], Y)
        ZB[north, 1, 1 : X + 1, PAD - 1, :] = to_col(LR[p, 4], X)
        ZB[0, 2, 1 : X + 1, PAD + Y, :] = to_col(LR[p, 5], X)

    straight = (0, 1, 2)
    folded = (3, 0, 2)

    V0 = V.at[0]
    for c in range(3):
        V0[c, 1 : X + 1, PAD : PAD + Y, :] = r_ref[c]
        C[c, 1 : X + 1, PAD : PAD + Y, :] = c_ref[c]
    stage(0, V0, straight)
    YS[5, 0, 0] = m_ref[1, :, Y - 1, :]
    YS[5, 0, 1] = c_ref[0, :, Y - 1, :]
    YS[5, 0, 2] = c_ref[2, :, Y - 1, :]

    pl.semaphore_wait(barrier, total - 1)
    coefs = [
        remote(m_ref.at[0, X - 1], MX, csend.at[0], crecv.at[0], dev(1, 0, 0)),
        remote(
            c_ref.at[pl.ds(1, 2), X - 1], C.at[pl.ds(1, 2), 0, loc], csend.at[1], crecv.at[1],
            dev(1, 0, 0),
        ),
        remote(YS.at[5, 0], YR.at[5, 0], csend.at[2], crecv.at[2], dev(0, 1, 0)),
        remote(m_ref.at[2], MZ, csend.at[3], crecv.at[3], dev(0, 0, 1)),
        remote(c_ref.at[pl.ds(0, 2)], CZ, csend.at[4], crecv.at[4], dev(0, 0, 1)),
    ]
    moving = launch(0, V0, ZV.at[0], 0)

    for copy in coefs:
        copy.wait_recv()
    C[0, 1 : X + 1, PAD - 1, :] = YR[5, 0, 1]
    C[2, 1 : X + 1, PAD - 1, :] = YR[5, 0, 2]

    @pl.loop(0, X)
    def _(i):
        p = i + 1
        c0, c1, c2 = (C[c, p, loc, :] for c in range(3))
        c0z, c1z = dn_z(c0, CZ[0, i]), dn_z(c1, CZ[1, i])
        low = pl.ds(PAD - 1, Y)
        m0, m1, m2 = (m_ref[c, i] for c in range(3))
        E[0, p, loc, :] = 1.0 / (m0 + c1 + c1z + c2 + C[2, p, low, :])
        E[1, p, loc, :] = 1.0 / (m1 + c2 + C[2, i, loc, :] + c0 + c0z)
        E[2, p, loc, :] = 1.0 / (m2 + c0 + C[0, p, low, :] + c1 + C[1, i, loc, :])
        before = jnp.where(i == 0, MX[...], m_ref[0, jnp.maximum(i - 1, 0)])
        back = YR[5, 0, 0, pl.ds(i, 1), :]
        m1y = jnp.where(row == 0, jnp.broadcast_to(back, (Y, Z)), pltpu.roll(m1, 1, 0))
        E[3, p, loc, :] = 1.0 / (m0 + before + m1 + m1y + m2 + dn_z(m2, MZ[i]))

    stage(1, E, folded)
    e_moving = launch(1, E, ZE, 1)
    land(0, V0, ZV.at[0], straight, moving)
    land(1, E, ZE, folded, e_moving)

    moments = {}
    full = pl.ds(0, Yh)
    full_up = pl.ds(1, Yh)
    low = pl.ds(PAD - 1, Y)
    high = pl.ds(PAD + 1, Y)
    hi_full = pl.ds(PAD, Yh)

    def fold(values):
        return jnp.sum(values.reshape(Y // 8, 8, Z), axis=0)

    for k in range(ITERS):
        W, ZW = V.at[k], ZV.at[k]
        if k:
            land(k + 1, W, ZW, straight, moving)

        def scaled(p, _):
            for c in range(3):
                S[c, p] = W[c, p] * E[c, p]
            return 0

        lax.fori_loop(0, X + 2, scaled, 0)

        def nodal(p, _):
            r2 = W[2, p, hi_full, :]
            q = (
                (W[0, p - 1, hi_full, :] - W[0, p, hi_full, :])
                + (W[1, p, pl.ds(PAD - 1, Yh), :] - W[1, p, hi_full, :])
                + (dn_z(r2, ZW[0, 2, p, hi_full, :]) - r2)
            )
            PH[p] = q * E[3, p, hi_full, :]
            return 0

        lax.fori_loop(1, X + 2, nodal, 0)

        def sz(side, c, p, rows):
            return ZW[side, c, p, rows, :] * ZE[side, c, p, rows, :]

        def curl_faces(p):
            s0, s1, s2 = (S[c, p, full, :] for c in range(3))
            g2 = C[2, p, full, :] * ((S[1, p + 1, full, :] - s1) - (S[0, p, full_up, :] - s0))
            t0, t2 = S[0, p, loc, :], S[2, p, loc, :]
            g1 = C[1, p, loc, :] * (
                (up_z(t0, sz(north, 0, p, loc)) - t0) - (S[2, p + 1, loc, :] - t2)
            )
            G[1, p, loc, :] = g1
            G[2, p, full, :] = g2
            return s1, s2

        curl_faces(0)

        def faces(p, _):
            s1, s2 = curl_faces(p)
            G[0, p, full, :] = C[0, p, full, :] * (
                (S[2, p, full_up, :] - s2) - (up_z(s1, sz(north, 1, p, full)) - s1)
            )
            return 0

        lax.fori_loop(1, X + 1, faces, 0)

        def apply(p, acc):
            i = p - 1
            s0, s1, s2 = (S[c, p, loc, :] for c in range(3))
            z0, z1, z2 = (sz(0, c, p, loc) for c in range(3))
            g0z = CZ[0, i] * ((sz(0, 2, p, high) - z2) - (pltpu.roll(s1, Z - 1, 1) - z1))
            g1z = CZ[1, i] * ((pltpu.roll(s0, Z - 1, 1) - z0) - (sz(0, 2, p + 1, loc) - z2))
            g0, g1, g2 = (G[c, p, loc, :] for c in range(3))
            g0b, g1b = dn_z(g0, g0z), dn_z(g1, g1z)
            n0 = ZW[north, 0, p, loc, :]
            n1 = ZW[north, 1, p, loc, :]
            qz = (
                (ZW[north, 0, i, loc, :] - n0)
                + (ZW[north, 1, p, low, :] - n1)
                + (pltpu.roll(W[2, p, loc, :], 1, 1) - ZW[north, 2, p, loc, :])
            )
            here = PH[p, 0:Y, :]
            b0 = s0 + (PH[p + 1, 0:Y, :] - here)
            b1 = s1 + (PH[p, 1 : Y + 1, :] - here)
            b2 = s2 + (up_z(here, qz * ZE[north, 3, p, loc, :]) - here)
            b = (b0, b1, b2)
            a = (
                (g1b - g1) - (G[2, p, low, :] - g2),
                (G[2, i, loc, :] - g2) - (g0b - g0),
                (G[0, p, low, :] - g0) - (G[1, i, loc, :] - g1),
            )
            w = [W[c, p, loc, :] for c in range(3)]
            v = [a[c] + (m_ref[c, i] * b[c] - SHIFT * w[c]) for c in range(3)]
            for c in range(3):
                BK[k, c, i] = b[c]
                if k + 1 < ITERS:
                    V[k + 1, c, p, loc, :] = v[c]
                else:
                    VL[c, i] = v[c]
            new = [acc[0] + fold(w[0] * b0 + w[1] * b1 + w[2] * b2)]
            for j in range(k + 1):
                bj = b if j == k else [BK[j, c, i] for c in range(3)]
                new.append(acc[j + 1] + fold(v[0] * bj[0] + v[1] * bj[1] + v[2] * bj[2]))
            return tuple(new)

        zero = jnp.zeros((8, Z), jnp.float32)
        acc = lax.fori_loop(1, X + 1, apply, (zero,) * (k + 2))
        moments[(k, k)] = acc[0]
        for j in range(k + 1):
            moments[(k + 1, j)] = acc[j + 1]
        if k + 1 < ITERS:
            stage(k + 2, V.at[k + 1], straight)
            moving = launch(k + 2, V.at[k + 1], ZV.at[k + 1], 0)

    keys = sorted(moments)
    line_lane = lax.broadcasted_iota(jnp.int32, (1, Z), 1)
    packed = jnp.zeros((1, Z), jnp.float32)
    for n, key in enumerate(keys):
        part = jnp.sum(jnp.sum(moments[key], axis=0, keepdims=True), axis=1, keepdims=True)
        packed = jnp.where(line_lane == n, part, packed)
    RED[rank] = packed

    def share(to, slot_from, o):
        return pltpu.make_async_remote_copy(
            src_ref=RED.at[slot_from], dst_ref=RED.at[slot_from], send_sem=rsend.at[o],
            recv_sem=rrecv.at[slot_from], device_id=ranked(to), device_id_type=MESH,
        )

    @pl.loop(1, total)
    def _(o):
        share(lax.rem(rank + o, total), rank, o).start()

    @pl.loop(1, total)
    def _(o):
        source = lax.rem(rank + o, total)
        share(source, source, o).wait_recv()

    summed = lax.fori_loop(0, total, lambda i, t: t + RED[i], jnp.zeros((1, Z), jnp.float32))
    gram = {}
    for n, (i, j) in enumerate(keys):
        value = jnp.sum(jnp.where(line_lane == n, summed, 0.0), axis=1, keepdims=True)
        gram[(i, j)] = value
        gram[(j, i)] = value

    def quad(left, right, entry):
        out = None
        for i, a in enumerate(left):
            for j, b in enumerate(right):
                term = (a * b) * entry(i, j)
                out = term if out is None else out + term
        return out

    one = jnp.ones((1, 1), jnp.float32)
    none = jnp.zeros((1, 1), jnp.float32)
    rho, pi, xi = [one], [], []
    gamma_old = alpha_old = None
    for k in range(ITERS):
        gamma = quad(rho, rho, lambda i, j: gram[(i, j)])
        delta = quad(rho, rho, lambda i, j: gram[(i + 1, j)] + SHIFT * gram[(i, j)])
        if k == 0:
            alpha = gamma / delta
            pi = list(rho)
        else:
            beta = gamma / gamma_old
            alpha = gamma / (delta - beta * gamma / alpha_old)
            pi = [rho[n] + beta * (pi[n] if n < len(pi) else none) for n in range(k + 1)]
        xi = [(xi[n] if n < len(xi) else none) + alpha * pi[n] for n in range(k + 1)]
        rho = rho + [none]
        moved = [none] * (k + 2)
        for n in range(k + 1):
            moved[n] = moved[n] + SHIFT * pi[n]
            moved[n + 1] = moved[n + 1] + pi[n]
        rho = [rho[n] - alpha * moved[n] for n in range(k + 2)]
        gamma_old, alpha_old = gamma, alpha

    spread = [jnp.broadcast_to(t, (Y, Z)) for t in rho]
    xspread = [jnp.broadcast_to(t, (Y, Z)) for t in xi]

    @pl.loop(0, X)
    def _(i):
        for c in range(3):
            res = spread[ITERS] * VL[c, i]
            sol = None
            for n in reversed(range(ITERS)):
                res = res + spread[n] * V[n, c, i + 1, loc, :]
                term = xspread[n] * BK[n, c, i]
                sol = term if sol is None else sol + term
            x_out[c, i] = sol
            res_out[c, i] = res

    for copy in pending:
        copy.wait_send()

    @pl.loop(1, total)
    def _(o):
        share(lax.rem(rank + o, total), rank, o).wait_send()


def body(sizes, right_side, mass_coef, curl_coef):
    _, X, Y, Z = right_side.shape
    nx, ny, nz = sizes
    total = nx * ny * nz
    sides = 1 if nz == 2 else 2
    XE, YE, Yh = X + 2, Y + 2 * PAD, Y + PAD
    f32 = jnp.float32
    vmem = pl.BlockSpec(memory_space=pltpu.VMEM)
    phases = ITERS + 1
    dma = pltpu.SemaphoreType.DMA
    return pl.pallas_call(
        functools.partial(kernel, sizes),
        out_shape=[jax.ShapeDtypeStruct(right_side.shape, f32)] * 2,
        in_specs=[vmem] * 3,
        out_specs=[vmem] * 2,
        scratch_shapes=[
            pltpu.VMEM((ITERS, 3, XE, YE, Z), f32),
            pltpu.VMEM((4, XE, YE, Z), f32),
            pltpu.VMEM((3, XE, YE, Z), f32),
            pltpu.VMEM((ITERS, sides, 3, XE, YE, Z), f32),
            pltpu.VMEM((sides, 4, XE, YE, Z), f32),
            pltpu.VMEM((2, X, Y, Z), f32),
            pltpu.VMEM((Y, Z), f32),
            pltpu.VMEM((X, Y, Z), f32),
            pltpu.VMEM((phases + 1, 2, 3, X, Z), f32),
            pltpu.VMEM((phases + 1, 2, 3, X, Z), f32),
            pltpu.VMEM((phases, 6, 1, Z), f32),
            pltpu.VMEM((phases, 6, 1, Z), f32),
            pltpu.VMEM((XE, Yh, Z), f32),
            pltpu.VMEM((3, XE, YE, Z), f32),
            pltpu.VMEM((3, XE, YE, Z), f32),
            pltpu.VMEM((ITERS, 3, X, Y, Z), f32),
            pltpu.VMEM((3, X, Y, Z), f32),
            pltpu.VMEM((total, 1, Z), f32),
            dma((phases, 10 + sides)),
            dma((phases, 10 + sides)),
            dma((5,)),
            dma((5,)),
            dma((total,)),
            dma((total,)),
        ],
        compiler_params=pltpu.CompilerParams(
            collective_id=0, has_side_effects=True, vmem_limit_bytes=56 * 1024 * 1024
        ),
        name="relayed_cg",
    )(right_side, mass_coef, curl_coef)


def solution(mesh):
    sizes = tuple(mesh.shape[a] for a in ("gx", "gy", "gz"))
    spec = P(None, "gx", "gy", "gz")
    return jax.shard_map(
        functools.partial(body, sizes), mesh=mesh, in_specs=(spec,) * 3, out_specs=(spec, spec),
        check_vma=False,
    )
```

```python
import functools

import jax
import jax.numpy as jnp
from jax import lax
from jax.experimental import pallas as pl
from jax.experimental.pallas import tpu as pltpu
from jax.sharding import PartitionSpec as P

ITERS = 4
UNROLL = True
PAD = 8
MESH = pl.DeviceIdType.MESH


def kernel(sizes, r_ref, m_ref, c_ref, x_out, res_out, V, E, C, ZV, ZE, CZ, MX, MZ, YS, YR, LS, LR,
           PH, S, G, ST, WL, RED, send, recv, csend, crecv, rsend, rrecv):
    nx, ny, nz = sizes
    total = nx * ny * nz
    _, X, Y, Z = r_ref.shape
    ix, iy, iz = (lax.axis_index(a) for a in ("gx", "gy", "gz"))
    rank = (ix * ny + iy) * nz + iz
    sides = ZV.shape[1]
    north = sides - 1
    Yh = Y + PAD
    YE = Y + 2 * PAD
    loc = pl.ds(PAD, Y)
    inx = pl.ds(1, X)

    def dev(dx, dy, dz):
        return (lax.rem(ix + dx + nx, nx), lax.rem(iy + dy + ny, ny), lax.rem(iz + dz + nz, nz))

    barrier = pltpu.get_barrier_semaphore()

    xs = [lax.rem(ix + d, nx) for d in range(nx)]
    ys = [lax.rem(iy + d, ny) for d in range(ny)]
    zs = [lax.rem(iz + d, nz) for d in range(nz)]
    others = [
        (a, b, c) for a in range(nx) for b in range(ny) for c in range(nz) if a or b or c
    ]
    for a, b, c in others:
        pl.semaphore_signal(barrier, inc=1, device_id=(xs[a], ys[b], zs[c]), device_id_type=MESH)

    lane = lax.broadcasted_iota(jnp.int32, (Y, Z), 1)
    row = lax.broadcasted_iota(jnp.int32, (Y, Z), 0)
    lane_h = lax.broadcasted_iota(jnp.int32, (Yh, Z), 1)
    pending = []

    def remote(src, dst, ss, rs, to):
        copy = pltpu.make_async_remote_copy(
            src_ref=src, dst_ref=dst, send_sem=ss, recv_sem=rs, device_id=to, device_id_type=MESH
        )
        copy.start()
        pending.append(copy)
        return copy

    def up_z(own, other):
        ln = lane if own.shape[0] == Y else lane_h
        return pltpu.roll(jnp.where(ln == 0, other, own), Z - 1, 1)

    def dn_z(own, other):
        ln = lane if own.shape[0] == Y else lane_h
        return pltpu.roll(jnp.where(ln == Z - 1, other, own), 1, 1)

    def to_row(col):
        n = col.shape[0]
        wide = jnp.broadcast_to(col, (n, Z))
        return jnp.sum(jnp.where(row[:n] == lane[:n], wide, 0.0), axis=0, keepdims=True)

    def to_col(line, n):
        wide = jnp.broadcast_to(line, (n, Z))
        col = jnp.sum(jnp.where(row[:n] == lane[:n], wide, 0.0), axis=1, keepdims=True)
        return jnp.broadcast_to(col, (n, Z))

    def stage(p, F, down_y):
        for c in range(3):
            YS[p, 0, c] = F[c, 1 : X + 1, PAD + Y - 1, :]
            YS[p, 1, c] = F[down_y[c], 1 : X + 1, PAD, :]
        LS[p, 0] = F[0, X, PAD : PAD + 1, :]
        LS[p, 1] = F[1, 1, PAD + Y - 1 : PAD + Y, :]
        LS[p, 2] = to_row(F[0, X, loc, :][:, 0:1])
        LS[p, 3] = to_row(F[2, 1, loc, :][:, Z - 1 : Z])
        LS[p, 4] = to_row(YS[p, 0, 1][:, 0:1])
        LS[p, 5] = to_row(YS[p, 1, 2][:, Z - 1 : Z])

    line_to = ((1, -1, 0), (-1, 1, 0), (1, 0, -1), (-1, 0, 1), (0, 1, -1), (0, -1, 1))

    def launch(p, F, ZB, down_x):
        def sem(n):
            return send.at[p, n], recv.at[p, n]

        out = [
            remote(F.at[pl.ds(0, 3), X, loc], F.at[pl.ds(0, 3), 0, loc], *sem(0), dev(1, 0, 0)),
            remote(
                F.at[pl.ds(down_x, 3), 1, loc], F.at[pl.ds(down_x, 3), X + 1, loc], *sem(1),
                dev(-1, 0, 0),
            ),
            remote(YS.at[p, 0], YR.at[p, 0], *sem(2), dev(0, 1, 0)),
            remote(YS.at[p, 1], YR.at[p, 1], *sem(3), dev(0, -1, 0)),
        ]
        for n in range(6):
            out.append(remote(LS.at[p, n], LR.at[p, n], *sem(4 + n), dev(*line_to[n])))
        for n in range(sides):
            out.append(
                remote(
                    F.at[:, inx, loc], ZB.at[n, :, inx, loc], *sem(10 + n),
                    dev(0, 0, 1 if n == 0 else -1),
                )
            )
        return out

    def land(p, F, ZB, down_y, copies):
        for copy in copies:
            copy.wait_recv()
        for c in range(3):
            F[c, 1 : X + 1, PAD - 1, :] = YR[p, 0, c]
            F[down_y[c], 1 : X + 1, PAD + Y, :] = YR[p, 1, c]
        F[0, 0, PAD + Y : PAD + Y + 1, :] = LR[p, 0]
        F[1, X + 1, PAD - 1 : PAD, :] = LR[p, 1]
        ZB[north, 0, 0, loc, :] = to_col(LR[p, 2], Y)
        ZB[0, 2, X + 1, loc, :] = to_col(LR[p, 3], Y)
        ZB[north, 1, 1 : X + 1, PAD - 1, :] = to_col(LR[p, 4], X)
        ZB[0, 2, 1 : X + 1, PAD + Y, :] = to_col(LR[p, 5], X)

    straight = (0, 1, 2)
    folded = (3, 0, 2)

    V0 = V.at[0]
    for c in range(3):
        V0[c, 1 : X + 1, PAD : PAD + Y, :] = r_ref[c]
        C[c, 1 : X + 1, PAD : PAD + Y, :] = c_ref[c]
    stage(0, V0, straight)
    YS[5, 0, 0] = m_ref[1, :, Y - 1, :]
    YS[5, 0, 1] = c_ref[0, :, Y - 1, :]
    YS[5, 0, 2] = c_ref[2, :, Y - 1, :]

    pl.semaphore_wait(barrier, total - 1)
    coefs = [
        remote(m_ref.at[0, X - 1], MX, csend.at[0], crecv.at[0], dev(1, 0, 0)),
        remote(
            c_ref.at[pl.ds(1, 2), X - 1], C.at[pl.ds(1, 2), 0, loc], csend.at[1], crecv.at[1],
            dev(1, 0, 0),
        ),
        remote(YS.at[5, 0], YR.at[5, 0], csend.at[2], crecv.at[2], dev(0, 1, 0)),
        remote(m_ref.at[2], MZ, csend.at[3], crecv.at[3], dev(0, 0, 1)),
        remote(c_ref.at[pl.ds(0, 2)], CZ, csend.at[4], crecv.at[4], dev(0, 0, 1)),
    ]
    moving = launch(0, V0, ZV.at[0], 0)

    for copy in coefs:
        copy.wait_recv()
    C[0, 1 : X + 1, PAD - 1, :] = YR[5, 0, 1]
    C[2, 1 : X + 1, PAD - 1, :] = YR[5, 0, 2]

    @pl.loop(0, X, unroll=UNROLL)
    def _(i):
        p = i + 1
        c0, c1, c2 = (C[c, p, loc, :] for c in range(3))
        c0z, c1z = dn_z(c0, CZ[0, i]), dn_z(c1, CZ[1, i])
        low = pl.ds(PAD - 1, Y)
        m0, m1, m2 = (m_ref[c, i] for c in range(3))
        E[0, p, loc, :] = 1.0 / (m0 + c1 + c1z + c2 + C[2, p, low, :])
        E[1, p, loc, :] = 1.0 / (m1 + c2 + C[2, i, loc, :] + c0 + c0z)
        E[2, p, loc, :] = 1.0 / (m2 + c0 + C[0, p, low, :] + c1 + C[1, i, loc, :])
        before = jnp.where(i == 0, MX[...], m_ref[0, jnp.maximum(i - 1, 0)])
        back = YR[5, 0, 0, pl.ds(i, 1), :]
        m1y = jnp.where(row == 0, jnp.broadcast_to(back, (Y, Z)), pltpu.roll(m1, 1, 0))
        E[3, p, loc, :] = 1.0 / (m0 + before + m1 + m1y + m2 + dn_z(m2, MZ[i]))

    stage(1, E, folded)
    e_moving = launch(1, E, ZE, 1)
    land(0, V0, ZV.at[0], straight, moving)
    land(1, E, ZE, folded, e_moving)

    line_lane = lax.broadcasted_iota(jnp.int32, (1, Z), 1)

    def share(k, n, slot):
        a, b, c = others[n]
        return pltpu.make_async_remote_copy(
            src_ref=RED.at[k, slot], dst_ref=RED.at[k, slot], send_sem=rsend.at[k, n],
            recv_sem=rrecv.at[k, slot], device_id=(xs[a], ys[b], zs[c]), device_id_type=MESH,
        )

    def start_sums(k, gamma, delta):
        packed = jnp.zeros((1, Z), jnp.float32)
        for n, value in enumerate((gamma, delta)):
            part = jnp.sum(jnp.sum(value, axis=0, keepdims=True), axis=1, keepdims=True)
            packed = jnp.where(line_lane == n, part, packed)
        RED[k, rank] = packed
        for n in range(len(others)):
            share(k, n, rank).start()

    def finish_sums(k):
        for n, (a, b, c) in enumerate(others):
            share(k, n, (xs[a] * ny + ys[b]) * nz + zs[c]).wait_recv()
        rows = [RED[k, n] for n in range(total)]
        while len(rows) > 1:
            rows = [sum(rows[n + 1 : n + 2], rows[n]) for n in range(0, len(rows), 2)]
        return [
            jnp.sum(jnp.where(line_lane == n, rows[0], 0.0), axis=1, keepdims=True)
            for n in range(2)
        ]

    gamma_old = alpha_old = None

    def step(k):
        gamma, delta = finish_sums(k)
        if k == 0:
            return gamma, gamma / delta, None
        beta = gamma / gamma_old
        return gamma, gamma / (delta - beta * gamma / alpha_old), beta

    full = pl.ds(0, Yh)
    full_up = pl.ds(1, Yh)
    low = pl.ds(PAD - 1, Y)
    high = pl.ds(PAD + 1, Y)
    hi_full = pl.ds(PAD, Yh)

    def fold(values):
        return jnp.sum(values.reshape(Y // 8, 8, Z), axis=0)

    for k in range(ITERS):
        W, ZW = V.at[k], ZV.at[k]
        if k:
            land(k + 1, W, ZW, straight, moving)

        def scaled(p, _):
            for c in range(3):
                S[c, p] = W[c, p] * E[c, p]
            return 0

        lax.fori_loop(0, X + 2, scaled, 0, unroll=UNROLL)

        def nodal(p, _):
            r2 = W[2, p, hi_full, :]
            q = (
                (W[0, p - 1, hi_full, :] - W[0, p, hi_full, :])
                + (W[1, p, pl.ds(PAD - 1, Yh), :] - W[1, p, hi_full, :])
                + (dn_z(r2, ZW[0, 2, p, hi_full, :]) - r2)
            )
            PH[p] = q * E[3, p, hi_full, :]
            return 0

        lax.fori_loop(1, X + 2, nodal, 0, unroll=UNROLL)

        def sz(side, c, p, rows):
            return ZW[side, c, p, rows, :] * ZE[side, c, p, rows, :]

        def curl_faces(p):
            s0, s1, s2 = (S[c, p, full, :] for c in range(3))
            g2 = C[2, p, full, :] * ((S[1, p + 1, full, :] - s1) - (S[0, p, full_up, :] - s0))
            t0, t2 = S[0, p, loc, :], S[2, p, loc, :]
            g1 = C[1, p, loc, :] * (
                (up_z(t0, sz(north, 0, p, loc)) - t0) - (S[2, p + 1, loc, :] - t2)
            )
            G[1, p, loc, :] = g1
            G[2, p, full, :] = g2
            return s1, s2

        curl_faces(0)

        def faces(p, _):
            s1, s2 = curl_faces(p)
            G[0, p, full, :] = C[0, p, full, :] * (
                (S[2, p, full_up, :] - s2) - (up_z(s1, sz(north, 1, p, full)) - s1)
            )
            return 0

        lax.fori_loop(1, X + 1, faces, 0, unroll=UNROLL)

        if k:
            gamma_old, alpha_old, beta = step(k - 1)
            alpha = jnp.broadcast_to(alpha_old, (Y, Z))
            if k > 1:
                beta = jnp.broadcast_to(beta, (Y, Z))

        def apply(p, acc):
            i = p - 1
            s0, s1, s2 = (S[c, p, loc, :] for c in range(3))
            z0, z1, z2 = (sz(0, c, p, loc) for c in range(3))
            g0z = CZ[0, i] * ((sz(0, 2, p, high) - z2) - (pltpu.roll(s1, Z - 1, 1) - z1))
            g1z = CZ[1, i] * ((pltpu.roll(s0, Z - 1, 1) - z0) - (sz(0, 2, p + 1, loc) - z2))
            g0, g1, g2 = (G[c, p, loc, :] for c in range(3))
            g0b, g1b = dn_z(g0, g0z), dn_z(g1, g1z)
            n0 = ZW[north, 0, p, loc, :]
            n1 = ZW[north, 1, p, loc, :]
            qz = (
                (ZW[north, 0, i, loc, :] - n0)
                + (ZW[north, 1, p, low, :] - n1)
                + (pltpu.roll(W[2, p, loc, :], 1, 1) - ZW[north, 2, p, loc, :])
            )
            here = PH[p, 0:Y, :]
            b0 = s0 + (PH[p + 1, 0:Y, :] - here)
            b1 = s1 + (PH[p, 1 : Y + 1, :] - here)
            b2 = s2 + (up_z(here, qz * ZE[north, 3, p, loc, :]) - here)
            b = (b0, b1, b2)
            a = (
                (g1b - g1) - (G[2, p, low, :] - g2),
                (G[2, i, loc, :] - g2) - (g0b - g0),
                (G[0, p, low, :] - g0) - (G[1, i, loc, :] - g1),
            )
            w = [W[c, p, loc, :] for c in range(3)]
            gamma, delta = acc
            terms = [[], []]
            for c in range(3):
                n = a[c] + m_ref[c, i] * b[c]
                if k == 0:
                    res, pre, img = w[c], b[c], n
                else:
                    u = ST[0, c, i]
                    prev = r_ref[c, i] if k == 1 else ST[6, c, i]
                    zz, qq, ss, pp = n, b[c], w[c], u
                    if k > 1:
                        zz = zz + beta * ST[1, c, i]
                        qq = qq + beta * ST[2, c, i]
                        ss = ss + beta * ST[3, c, i]
                        pp = pp + beta * ST[4, c, i]
                    if k + 1 < ITERS:
                        ST[1, c, i] = zz
                        ST[2, c, i] = qq
                    ST[3, c, i] = ss
                    ST[4, c, i] = pp
                    ST[5, c, i] = alpha * pp if k == 1 else ST[5, c, i] + alpha * pp
                    res, pre, img = prev - alpha * ss, u - alpha * qq, w[c] - alpha * zz
                    ST[6, c, i] = res
                ST[0, c, i] = pre
                if k + 1 < ITERS:
                    V[k + 1, c, p, loc, :] = img
                else:
                    WL[c, i] = img
                terms[0].append(res * pre)
                terms[1].append(img * pre)
            return (
                gamma + fold(terms[0][0] + terms[0][1] + terms[0][2]),
                delta + fold(terms[1][0] + terms[1][1] + terms[1][2]),
            )

        zero = jnp.zeros((8, Z), jnp.float32)
        gamma, delta = lax.fori_loop(1, X + 1, apply, (zero, zero), unroll=UNROLL)
        if k + 1 < ITERS:
            stage(k + 2, V.at[k + 1], straight)
            moving = launch(k + 2, V.at[k + 1], ZV.at[k + 1], 0)
        start_sums(k, gamma, delta)

    _, alpha, beta = step(ITERS - 1)
    alpha = jnp.broadcast_to(alpha, (Y, Z))
    beta = jnp.broadcast_to(beta, (Y, Z))

    @pl.loop(0, X, unroll=UNROLL)
    def _(i):
        for c in range(3):
            x_out[c, i] = ST[5, c, i] + alpha * (ST[0, c, i] + beta * ST[4, c, i])
            res_out[c, i] = ST[6, c, i] - alpha * (WL[c, i] + beta * ST[3, c, i])

    for copy in pending:
        copy.wait_send()
    for k in range(ITERS):
        for n in range(len(others)):
            share(k, n, rank).wait_send()


def body(sizes, right_side, mass_coef, curl_coef):
    _, X, Y, Z = right_side.shape
    nx, ny, nz = sizes
    total = nx * ny * nz
    sides = 1 if nz == 2 else 2
    XE, YE, Yh = X + 2, Y + 2 * PAD, Y + PAD
    f32 = jnp.float32
    vmem = pl.BlockSpec(memory_space=pltpu.VMEM)
    phases = ITERS + 1
    dma = pltpu.SemaphoreType.DMA
    return pl.pallas_call(
        functools.partial(kernel, sizes),
        out_shape=[jax.ShapeDtypeStruct(right_side.shape, f32)] * 2,
        in_specs=[vmem] * 3,
        out_specs=[vmem] * 2,
        scratch_shapes=[
            pltpu.VMEM((ITERS, 3, XE, YE, Z), f32),
            pltpu.VMEM((4, XE, YE, Z), f32),
            pltpu.VMEM((3, XE, YE, Z), f32),
            pltpu.VMEM((ITERS, sides, 3, XE, YE, Z), f32),
            pltpu.VMEM((sides, 4, XE, YE, Z), f32),
            pltpu.VMEM((2, X, Y, Z), f32),
            pltpu.VMEM((Y, Z), f32),
            pltpu.VMEM((X, Y, Z), f32),
            pltpu.VMEM((phases + 1, 2, 3, X, Z), f32),
            pltpu.VMEM((phases + 1, 2, 3, X, Z), f32),
            pltpu.VMEM((phases, 6, 1, Z), f32),
            pltpu.VMEM((phases, 6, 1, Z), f32),
            pltpu.VMEM((XE, Yh, Z), f32),
            pltpu.VMEM((3, XE, YE, Z), f32),
            pltpu.VMEM((3, XE, YE, Z), f32),
            pltpu.VMEM((7, 3, X, Y, Z), f32),
            pltpu.VMEM((3, X, Y, Z), f32),
            pltpu.VMEM((ITERS, total, 1, Z), f32),
            dma((phases, 10 + sides)),
            dma((phases, 10 + sides)),
            dma((5,)),
            dma((5,)),
            dma((ITERS, total)),
            dma((ITERS, total)),
        ],
        compiler_params=pltpu.CompilerParams(
            collective_id=0, has_side_effects=True, vmem_limit_bytes=24 * 1024 * 1024
        ),
        name="relayed_cg",
    )(right_side, mass_coef, curl_coef)


def solution(mesh):
    sizes = tuple(mesh.shape[a] for a in ("gx", "gy", "gz"))
    spec = P(None, "gx", "gy", "gz")
    return jax.shard_map(
        functools.partial(body, sizes), mesh=mesh, in_specs=(spec,) * 3, out_specs=(spec, spec),
        check_vma=False,
    )
```

```python
import functools

import jax
import jax.numpy as jnp
from jax import lax
from jax.experimental import pallas as pl
from jax.experimental.pallas import tpu as pltpu
from jax.sharding import PartitionSpec as P

ITERS = 4
UNROLL = True
PAD = 8
MESH = pl.DeviceIdType.MESH


def kernel(sizes, r_hbm, m_hbm, c_hbm, x_out, res_out, V, E, C, ZV, ZE, CZ, MX, MZ, YS, YR, LS, LR,
           PH, S, G, ST, WL, RED, send, recv, csend, crecv, rsend, rrecv,
           m_ref, lsem):
    nx, ny, nz = sizes
    total = nx * ny * nz
    _, X, Y, Z = m_ref.shape
    ix, iy, iz = (lax.axis_index(a) for a in ("gx", "gy", "gz"))
    rank = (ix * ny + iy) * nz + iz
    sides = ZV.shape[1]
    north = sides - 1
    Yh = Y + PAD
    YE = Y + 2 * PAD
    loc = pl.ds(PAD, Y)
    inx = pl.ds(1, X)

    def dev(dx, dy, dz):
        return (lax.rem(ix + dx + nx, nx), lax.rem(iy + dy + ny, ny), lax.rem(iz + dz + nz, nz))

    loads = [
        pltpu.make_async_copy(m_hbm, m_ref, lsem.at[0]),
        pltpu.make_async_copy(c_hbm, C.at[:, inx, loc], lsem.at[1]),
        pltpu.make_async_copy(r_hbm, V.at[0, :, inx, loc], lsem.at[2]),
    ]
    for load in loads:
        load.start()
    barrier = pltpu.get_barrier_semaphore()

    xs = [lax.rem(ix + d, nx) for d in range(nx)]
    ys = [lax.rem(iy + d, ny) for d in range(ny)]
    zs = [lax.rem(iz + d, nz) for d in range(nz)]
    others = [
        (a, b, c) for a in range(nx) for b in range(ny) for c in range(nz) if a or b or c
    ]
    for a, b, c in others:
        pl.semaphore_signal(barrier, inc=1, device_id=(xs[a], ys[b], zs[c]), device_id_type=MESH)

    lane = lax.broadcasted_iota(jnp.int32, (Y, Z), 1)
    row = lax.broadcasted_iota(jnp.int32, (Y, Z), 0)
    lane_h = lax.broadcasted_iota(jnp.int32, (Yh, Z), 1)
    pending = []

    def remote(src, dst, ss, rs, to):
        copy = pltpu.make_async_remote_copy(
            src_ref=src, dst_ref=dst, send_sem=ss, recv_sem=rs, device_id=to, device_id_type=MESH
        )
        copy.start()
        pending.append(copy)
        return copy

    def up_z(own, other):
        ln = lane if own.shape[0] == Y else lane_h
        return pltpu.roll(jnp.where(ln == 0, other, own), Z - 1, 1)

    def dn_z(own, other):
        ln = lane if own.shape[0] == Y else lane_h
        return pltpu.roll(jnp.where(ln == Z - 1, other, own), 1, 1)

    def to_row(col):
        n = col.shape[0]
        wide = jnp.broadcast_to(col, (n, Z))
        return jnp.sum(jnp.where(row[:n] == lane[:n], wide, 0.0), axis=0, keepdims=True)

    def to_col(line, n):
        wide = jnp.broadcast_to(line, (n, Z))
        col = jnp.sum(jnp.where(row[:n] == lane[:n], wide, 0.0), axis=1, keepdims=True)
        return jnp.broadcast_to(col, (n, Z))

    def stage(p, F, down_y):
        for c in range(3):
            YS[p, 0, c] = F[c, 1 : X + 1, PAD + Y - 1, :]
            YS[p, 1, c] = F[down_y[c], 1 : X + 1, PAD, :]
        LS[p, 0] = F[0, X, PAD : PAD + 1, :]
        LS[p, 1] = F[1, 1, PAD + Y - 1 : PAD + Y, :]
        LS[p, 2] = to_row(F[0, X, loc, :][:, 0:1])
        LS[p, 3] = to_row(F[2, 1, loc, :][:, Z - 1 : Z])
        LS[p, 4] = to_row(YS[p, 0, 1][:, 0:1])
        LS[p, 5] = to_row(YS[p, 1, 2][:, Z - 1 : Z])

    line_to = ((1, -1, 0), (-1, 1, 0), (1, 0, -1), (-1, 0, 1), (0, 1, -1), (0, -1, 1))

    def launch(p, F, ZB, down_x, between=lambda: None):
        def sem(n):
            return send.at[p, n], recv.at[p, n]

        out = []
        for n in range(6):
            out.append(remote(LS.at[p, n], LR.at[p, n], *sem(4 + n), dev(*line_to[n])))
        out.append(remote(YS.at[p, 0], YR.at[p, 0], *sem(2), dev(0, 1, 0)))
        out.append(remote(YS.at[p, 1], YR.at[p, 1], *sem(3), dev(0, -1, 0)))
        for n in range(sides):
            out.append(
                remote(
                    F.at[:, inx, loc], ZB.at[n, :, inx, loc], *sem(10 + n),
                    dev(0, 0, 1 if n == 0 else -1),
                )
            )
        between()
        out.append(
            remote(F.at[pl.ds(0, 3), X, loc], F.at[pl.ds(0, 3), 0, loc], *sem(0), dev(1, 0, 0))
        )
        out.append(
            remote(
                F.at[pl.ds(down_x, 3), 1, loc], F.at[pl.ds(down_x, 3), X + 1, loc], *sem(1),
                dev(-1, 0, 0),
            )
        )
        return out

    def land(p, F, ZB, down_y, copies):
        for copy in copies:
            copy.wait_recv()
        for c in range(3):
            F[c, 1 : X + 1, PAD - 1, :] = YR[p, 0, c]
            F[down_y[c], 1 : X + 1, PAD + Y, :] = YR[p, 1, c]
        F[0, 0, PAD + Y : PAD + Y + 1, :] = LR[p, 0]
        F[1, X + 1, PAD - 1 : PAD, :] = LR[p, 1]
        ZB[north, 0, 0, loc, :] = to_col(LR[p, 2], Y)
        ZB[0, 2, X + 1, loc, :] = to_col(LR[p, 3], Y)
        ZB[north, 1, 1 : X + 1, PAD - 1, :] = to_col(LR[p, 4], X)
        ZB[0, 2, 1 : X + 1, PAD + Y, :] = to_col(LR[p, 5], X)

    straight = (0, 1, 2)
    folded = (3, 0, 2)

    V0 = V.at[0]
    for load in loads:
        load.wait()
    YS[5, 0, 0] = m_ref[1, :, Y - 1, :]
    YS[5, 0, 1] = C[0, 1 : X + 1, PAD + Y - 1, :]
    YS[5, 0, 2] = C[2, 1 : X + 1, PAD + Y - 1, :]
    stage(0, V0, straight)

    pl.semaphore_wait(barrier, total - 1)
    coefs = [
        remote(YS.at[5, 0], YR.at[5, 0], csend.at[2], crecv.at[2], dev(0, 1, 0)),
        remote(m_ref.at[2], MZ, csend.at[3], crecv.at[3], dev(0, 0, 1)),
        remote(C.at[pl.ds(0, 2), inx, loc], CZ, csend.at[4], crecv.at[4], dev(0, 0, 1)),
        remote(m_ref.at[0, X - 1], MX, csend.at[0], crecv.at[0], dev(1, 0, 0)),
        remote(
            C.at[pl.ds(1, 2), X, loc], C.at[pl.ds(1, 2), 0, loc], csend.at[1], crecv.at[1],
            dev(1, 0, 0),
        ),
    ]
    moving = launch(0, V0, ZV.at[0], 0)

    for copy in coefs:
        copy.wait_recv()
    C[0, 1 : X + 1, PAD - 1, :] = YR[5, 0, 1]
    C[2, 1 : X + 1, PAD - 1, :] = YR[5, 0, 2]

    @pl.loop(0, X, unroll=UNROLL)
    def _(i):
        p = i + 1
        c0, c1, c2 = (C[c, p, loc, :] for c in range(3))
        c0z, c1z = dn_z(c0, CZ[0, i]), dn_z(c1, CZ[1, i])
        low = pl.ds(PAD - 1, Y)
        m0, m1, m2 = (m_ref[c, i] for c in range(3))
        E[0, p, loc, :] = 1.0 / (m0 + c1 + c1z + c2 + C[2, p, low, :])
        E[1, p, loc, :] = 1.0 / (m1 + c2 + C[2, i, loc, :] + c0 + c0z)
        E[2, p, loc, :] = 1.0 / (m2 + c0 + C[0, p, low, :] + c1 + C[1, i, loc, :])
        before = jnp.where(i == 0, MX[...], m_ref[0, jnp.maximum(i - 1, 0)])
        back = YR[5, 0, 0, pl.ds(i, 1), :]
        m1y = jnp.where(row == 0, jnp.broadcast_to(back, (Y, Z)), pltpu.roll(m1, 1, 0))
        E[3, p, loc, :] = 1.0 / (m0 + before + m1 + m1y + m2 + dn_z(m2, MZ[i]))

    stage(1, E, folded)
    e_moving = launch(1, E, ZE, 1)
    land(0, V0, ZV.at[0], straight, moving)
    land(1, E, ZE, folded, e_moving)

    line_lane = lax.broadcasted_iota(jnp.int32, (1, Z), 1)

    def share(k, n, slot):
        a, b, c = others[n]
        return pltpu.make_async_remote_copy(
            src_ref=RED.at[k, slot], dst_ref=RED.at[k, slot], send_sem=rsend.at[k, n],
            recv_sem=rrecv.at[k, slot], device_id=(xs[a], ys[b], zs[c]), device_id_type=MESH,
        )

    def start_sums(k, gamma, delta):
        packed = jnp.zeros((1, Z), jnp.float32)
        for n, value in enumerate((gamma, delta)):
            part = jnp.sum(jnp.sum(value, axis=0, keepdims=True), axis=1, keepdims=True)
            packed = jnp.where(line_lane == n, part, packed)
        RED[k, rank] = packed
        for n in range(len(others)):
            share(k, n, rank).start()

    def finish_sums(k):
        for n, (a, b, c) in enumerate(others):
            share(k, n, (xs[a] * ny + ys[b]) * nz + zs[c]).wait_recv()
        rows = [RED[k, n] for n in range(total)]
        while len(rows) > 1:
            rows = [sum(rows[n + 1 : n + 2], rows[n]) for n in range(0, len(rows), 2)]
        return [
            jnp.sum(jnp.where(line_lane == n, rows[0], 0.0), axis=1, keepdims=True)
            for n in range(2)
        ]

    gamma_old = alpha_old = None

    def step(k):
        gamma, delta = finish_sums(k)
        if k == 0:
            return gamma, gamma / delta, None
        beta = gamma / gamma_old
        return gamma, gamma / (delta - beta * gamma / alpha_old), beta

    full = pl.ds(0, Yh)
    full_up = pl.ds(1, Yh)
    low = pl.ds(PAD - 1, Y)
    high = pl.ds(PAD + 1, Y)
    hi_full = pl.ds(PAD, Yh)

    def fold(values):
        return jnp.sum(values.reshape(Y // 8, 8, Z), axis=0)

    for k in range(ITERS):
        W, ZW = V.at[k], ZV.at[k]
        if k:
            land(k + 1, W, ZW, straight, moving)

        def scaled(p, _):
            for c in range(3):
                S[c, p] = W[c, p] * E[c, p]
            return 0

        lax.fori_loop(0, X + 2, scaled, 0, unroll=UNROLL)

        def nodal(p, _):
            r2 = W[2, p, hi_full, :]
            q = (
                (W[0, p - 1, hi_full, :] - W[0, p, hi_full, :])
                + (W[1, p, pl.ds(PAD - 1, Yh), :] - W[1, p, hi_full, :])
                + (dn_z(r2, ZW[0, 2, p, hi_full, :]) - r2)
            )
            PH[p] = q * E[3, p, hi_full, :]
            return 0

        lax.fori_loop(1, X + 2, nodal, 0, unroll=UNROLL)

        def sz(side, c, p, rows):
            return ZW[side, c, p, rows, :] * ZE[side, c, p, rows, :]

        def curl_faces(p):
            s0, s1, s2 = (S[c, p, full, :] for c in range(3))
            g2 = C[2, p, full, :] * ((S[1, p + 1, full, :] - s1) - (S[0, p, full_up, :] - s0))
            t0, t2 = S[0, p, loc, :], S[2, p, loc, :]
            g1 = C[1, p, loc, :] * (
                (up_z(t0, sz(north, 0, p, loc)) - t0) - (S[2, p + 1, loc, :] - t2)
            )
            G[1, p, loc, :] = g1
            G[2, p, full, :] = g2
            return s1, s2

        curl_faces(0)

        def faces(p, _):
            s1, s2 = curl_faces(p)
            G[0, p, full, :] = C[0, p, full, :] * (
                (S[2, p, full_up, :] - s2) - (up_z(s1, sz(north, 1, p, full)) - s1)
            )
            return 0

        lax.fori_loop(1, X + 1, faces, 0, unroll=UNROLL)

        if k:
            gamma_old, alpha_old, beta = step(k - 1)
            alpha = jnp.broadcast_to(alpha_old, (Y, Z))
            if k > 1:
                beta = jnp.broadcast_to(beta, (Y, Z))

        def apply(p, acc):
            i = p - 1
            s0, s1, s2 = (S[c, p, loc, :] for c in range(3))
            z0, z1, z2 = (sz(0, c, p, loc) for c in range(3))
            g0z = CZ[0, i] * ((sz(0, 2, p, high) - z2) - (pltpu.roll(s1, Z - 1, 1) - z1))
            g1z = CZ[1, i] * ((pltpu.roll(s0, Z - 1, 1) - z0) - (sz(0, 2, p + 1, loc) - z2))
            g0, g1, g2 = (G[c, p, loc, :] for c in range(3))
            g0b, g1b = dn_z(g0, g0z), dn_z(g1, g1z)
            n0 = ZW[north, 0, p, loc, :]
            n1 = ZW[north, 1, p, loc, :]
            qz = (
                (ZW[north, 0, i, loc, :] - n0)
                + (ZW[north, 1, p, low, :] - n1)
                + (pltpu.roll(W[2, p, loc, :], 1, 1) - ZW[north, 2, p, loc, :])
            )
            here = PH[p, 0:Y, :]
            b0 = s0 + (PH[p + 1, 0:Y, :] - here)
            b1 = s1 + (PH[p, 1 : Y + 1, :] - here)
            b2 = s2 + (up_z(here, qz * ZE[north, 3, p, loc, :]) - here)
            b = (b0, b1, b2)
            a = (
                (g1b - g1) - (G[2, p, low, :] - g2),
                (G[2, i, loc, :] - g2) - (g0b - g0),
                (G[0, p, low, :] - g0) - (G[1, i, loc, :] - g1),
            )
            w = [W[c, p, loc, :] for c in range(3)]
            gamma, delta = acc
            terms = [[], []]
            for c in range(3):
                n = a[c] + m_ref[c, i] * b[c]
                if k == 0:
                    res, pre, img = w[c], b[c], n
                else:
                    u = ST[0, c, i]
                    prev = V[0, c, p, loc, :] if k == 1 else ST[6, c, i]
                    zz, qq, ss, pp = n, b[c], w[c], u
                    if k > 1:
                        zz = zz + beta * ST[1, c, i]
                        qq = qq + beta * ST[2, c, i]
                        ss = ss + beta * ST[3, c, i]
                        pp = pp + beta * ST[4, c, i]
                    if k + 1 < ITERS:
                        ST[1, c, i] = zz
                        ST[2, c, i] = qq
                    ST[3, c, i] = ss
                    ST[4, c, i] = pp
                    ST[5, c, i] = alpha * pp if k == 1 else ST[5, c, i] + alpha * pp
                    res, pre, img = prev - alpha * ss, u - alpha * qq, w[c] - alpha * zz
                    ST[6, c, i] = res
                ST[0, c, i] = pre
                if k + 1 < ITERS:
                    V[k + 1, c, p, loc, :] = img
                else:
                    WL[c, i] = img
                terms[0].append(res * pre)
                terms[1].append(img * pre)
            return (
                gamma + fold(terms[0][0] + terms[0][1] + terms[0][2]),
                delta + fold(terms[1][0] + terms[1][1] + terms[1][2]),
            )

        zero = jnp.zeros((8, Z), jnp.float32)
        gamma, delta = lax.fori_loop(1, X + 1, apply, (zero, zero), unroll=UNROLL)
        if k + 1 < ITERS:
            stage(k + 2, V.at[k + 1], straight)
            moving = launch(
                k + 2, V.at[k + 1], ZV.at[k + 1], 0, lambda: start_sums(k, gamma, delta)
            )
        else:
            start_sums(k, gamma, delta)

    _, alpha, beta = step(ITERS - 1)
    alpha = jnp.broadcast_to(alpha, (Y, Z))
    beta = jnp.broadcast_to(beta, (Y, Z))

    @pl.loop(0, X, unroll=UNROLL)
    def _(i):
        for c in range(3):
            x_out[c, i] = ST[5, c, i] + alpha * (ST[0, c, i] + beta * ST[4, c, i])
            res_out[c, i] = ST[6, c, i] - alpha * (WL[c, i] + beta * ST[3, c, i])

    for copy in pending:
        copy.wait_send()
    for k in range(ITERS):
        for n in range(len(others)):
            share(k, n, rank).wait_send()


def body(sizes, right_side, mass_coef, curl_coef):
    _, X, Y, Z = right_side.shape
    nx, ny, nz = sizes
    total = nx * ny * nz
    sides = 1 if nz == 2 else 2
    XE, YE, Yh = X + 2, Y + 2 * PAD, Y + PAD
    f32 = jnp.float32
    vmem = pl.BlockSpec(memory_space=pltpu.VMEM)
    phases = ITERS + 1
    dma = pltpu.SemaphoreType.DMA
    return pl.pallas_call(
        functools.partial(kernel, sizes),
        out_shape=[jax.ShapeDtypeStruct(right_side.shape, f32)] * 2,
        in_specs=[pl.BlockSpec(memory_space=pltpu.HBM)] * 3,
        out_specs=[vmem] * 2,
        scratch_shapes=[
            pltpu.VMEM((ITERS, 3, XE, YE, Z), f32),
            pltpu.VMEM((4, XE, YE, Z), f32),
            pltpu.VMEM((3, XE, YE, Z), f32),
            pltpu.VMEM((ITERS, sides, 3, XE, YE, Z), f32),
            pltpu.VMEM((sides, 4, XE, YE, Z), f32),
            pltpu.VMEM((2, X, Y, Z), f32),
            pltpu.VMEM((Y, Z), f32),
            pltpu.VMEM((X, Y, Z), f32),
            pltpu.VMEM((phases + 1, 2, 3, X, Z), f32),
            pltpu.VMEM((phases + 1, 2, 3, X, Z), f32),
            pltpu.VMEM((phases, 6, 1, Z), f32),
            pltpu.VMEM((phases, 6, 1, Z), f32),
            pltpu.VMEM((XE, Yh, Z), f32),
            pltpu.VMEM((3, XE, YE, Z), f32),
            pltpu.VMEM((3, XE, YE, Z), f32),
            pltpu.VMEM((7, 3, X, Y, Z), f32),
            pltpu.VMEM((3, X, Y, Z), f32),
            pltpu.VMEM((ITERS, total, 1, Z), f32),
            dma((phases, 10 + sides)),
            dma((phases, 10 + sides)),
            dma((5,)),
            dma((5,)),
            dma((ITERS, total)),
            dma((ITERS, total)),
            pltpu.VMEM((3, X, Y, Z), f32),
            dma((3,)),
        ],
        compiler_params=pltpu.CompilerParams(
            collective_id=0, has_side_effects=True, vmem_limit_bytes=24 * 1024 * 1024
        ),
        name="relayed_cg",
    )(*(pltpu.with_memory_space_constraint(a, pltpu.HBM) for a in (right_side, mass_coef, curl_coef)))


def solution(mesh):
    sizes = tuple(mesh.shape[a] for a in ("gx", "gy", "gz"))
    spec = P(None, "gx", "gy", "gz")
    return jax.shard_map(
        functools.partial(body, sizes), mesh=mesh, in_specs=(spec,) * 3, out_specs=(spec, spec),
        check_vma=False,
    )
```

```python
import functools

import jax
import jax.numpy as jnp
from jax import lax
from jax.experimental import pallas as pl
from jax.experimental.pallas import tpu as pltpu
from jax.sharding import PartitionSpec as P

ITERS = 4
UNROLL = True
PAD = 8
MESH = pl.DeviceIdType.MESH


def kernel(sizes, r_hbm, m_hbm, c_hbm, x_out, res_out, V, E, C, ZV, ZE, CZ, MX, MZ, YS, YR, LS, LR,
           PH, S, G, ST, WL, RED, send, recv, csend, crecv, rsend, rrecv,
           m_ref, lsem):
    nx, ny, nz = sizes
    total = nx * ny * nz
    _, X, Y, Z = m_ref.shape
    ix, iy, iz = (lax.axis_index(a) for a in ("gx", "gy", "gz"))
    rank = (ix * ny + iy) * nz + iz
    sides = ZV.shape[1]
    north = sides - 1
    Yh = Y + PAD
    YE = Y + 2 * PAD
    loc = pl.ds(PAD, Y)
    inx = pl.ds(1, X)

    def dev(dx, dy, dz):
        return (lax.rem(ix + dx + nx, nx), lax.rem(iy + dy + ny, ny), lax.rem(iz + dz + nz, nz))

    loads = [
        pltpu.make_async_copy(m_hbm, m_ref, lsem.at[0]),
        pltpu.make_async_copy(c_hbm, C.at[:, inx, loc], lsem.at[1]),
        pltpu.make_async_copy(r_hbm, V.at[0, :, inx, loc], lsem.at[2]),
    ]
    for load in loads:
        load.start()
    barrier = pltpu.get_barrier_semaphore()

    xs = [lax.rem(ix + d, nx) for d in range(nx)]
    ys = [lax.rem(iy + d, ny) for d in range(ny)]
    zs = [lax.rem(iz + d, nz) for d in range(nz)]
    others = [
        (a, b, c) for a in range(nx) for b in range(ny) for c in range(nz) if a or b or c
    ]
    for a, b, c in others:
        pl.semaphore_signal(barrier, inc=1, device_id=(xs[a], ys[b], zs[c]), device_id_type=MESH)

    lane = lax.broadcasted_iota(jnp.int32, (Y, Z), 1)
    row = lax.broadcasted_iota(jnp.int32, (Y, Z), 0)
    lane_h = lax.broadcasted_iota(jnp.int32, (Yh, Z), 1)
    pending = []

    def remote(src, dst, ss, rs, to):
        copy = pltpu.make_async_remote_copy(
            src_ref=src, dst_ref=dst, send_sem=ss, recv_sem=rs, device_id=to, device_id_type=MESH
        )
        copy.start()
        pending.append(copy)
        return copy

    def up_z(own, other):
        ln = lane if own.shape[0] == Y else lane_h
        return pltpu.roll(jnp.where(ln == 0, other, own), Z - 1, 1)

    def dn_z(own, other):
        ln = lane if own.shape[0] == Y else lane_h
        return pltpu.roll(jnp.where(ln == Z - 1, other, own), 1, 1)

    def to_row(col):
        n = col.shape[0]
        wide = jnp.broadcast_to(col, (n, Z))
        return jnp.sum(jnp.where(row[:n] == lane[:n], wide, 0.0), axis=0, keepdims=True)

    def to_col(line, n):
        wide = jnp.broadcast_to(line, (n, Z))
        col = jnp.sum(jnp.where(row[:n] == lane[:n], wide, 0.0), axis=1, keepdims=True)
        return jnp.broadcast_to(col, (n, Z))

    def stage(p, F, down_y):
        for c in range(3):
            YS[p, 0, c] = F[c, 1 : X + 1, PAD + Y - 1, :]
            YS[p, 1, c] = F[down_y[c], 1 : X + 1, PAD, :]
        LS[p, 0] = F[0, X, PAD : PAD + 1, :]
        LS[p, 1] = F[1, 1, PAD + Y - 1 : PAD + Y, :]
        LS[p, 2] = to_row(F[0, X, loc, :][:, 0:1])
        LS[p, 3] = to_row(F[2, 1, loc, :][:, Z - 1 : Z])
        LS[p, 4] = to_row(YS[p, 0, 1][:, 0:1])
        LS[p, 5] = to_row(YS[p, 1, 2][:, Z - 1 : Z])

    line_to = ((1, -1, 0), (-1, 1, 0), (1, 0, -1), (-1, 0, 1), (0, 1, -1), (0, -1, 1))

    def launch(p, F, ZB, down_x, between=lambda: None):
        def sem(n):
            return send.at[p, n], recv.at[p, n]

        out = []
        for n in range(6):
            out.append(remote(LS.at[p, n], LR.at[p, n], *sem(4 + n), dev(*line_to[n])))
        out.append(remote(YS.at[p, 0], YR.at[p, 0], *sem(2), dev(0, 1, 0)))
        out.append(remote(YS.at[p, 1], YR.at[p, 1], *sem(3), dev(0, -1, 0)))
        for n in range(sides):
            out.append(
                remote(
                    F.at[:, inx, loc], ZB.at[n, :, inx, loc], *sem(10 + n),
                    dev(0, 0, 1 if n == 0 else -1),
                )
            )
        between()
        out.append(
            remote(F.at[pl.ds(0, 3), X, loc], F.at[pl.ds(0, 3), 0, loc], *sem(0), dev(1, 0, 0))
        )
        out.append(
            remote(
                F.at[pl.ds(down_x, 3), 1, loc], F.at[pl.ds(down_x, 3), X + 1, loc], *sem(1),
                dev(-1, 0, 0),
            )
        )
        return out

    def land(p, F, ZB, down_y, copies):
        for copy in copies:
            copy.wait_recv()
        for c in range(3):
            F[c, 1 : X + 1, PAD - 1, :] = YR[p, 0, c]
            F[down_y[c], 1 : X + 1, PAD + Y, :] = YR[p, 1, c]
        F[0, 0, PAD + Y : PAD + Y + 1, :] = LR[p, 0]
        F[1, X + 1, PAD - 1 : PAD, :] = LR[p, 1]
        ZB[north, 0, 0, loc, :] = to_col(LR[p, 2], Y)
        ZB[0, 2, X + 1, loc, :] = to_col(LR[p, 3], Y)
        ZB[north, 1, 1 : X + 1, PAD - 1, :] = to_col(LR[p, 4], X)
        ZB[0, 2, 1 : X + 1, PAD + Y, :] = to_col(LR[p, 5], X)

    straight = (0, 1, 2)
    folded = (3, 0, 2)

    V0 = V.at[0]
    for load in loads:
        load.wait()
    YS[5, 0, 0] = m_ref[1, :, Y - 1, :]
    YS[5, 0, 1] = C[0, 1 : X + 1, PAD + Y - 1, :]
    YS[5, 0, 2] = C[2, 1 : X + 1, PAD + Y - 1, :]
    stage(0, V0, straight)

    pl.semaphore_wait(barrier, total - 1)
    coefs = [
        remote(YS.at[5, 0], YR.at[5, 0], csend.at[2], crecv.at[2], dev(0, 1, 0)),
        remote(m_ref.at[2], MZ, csend.at[3], crecv.at[3], dev(0, 0, 1)),
        remote(C.at[pl.ds(0, 2), inx, loc], CZ, csend.at[4], crecv.at[4], dev(0, 0, 1)),
        remote(m_ref.at[0, X - 1], MX, csend.at[0], crecv.at[0], dev(1, 0, 0)),
        remote(
            C.at[pl.ds(1, 2), X, loc], C.at[pl.ds(1, 2), 0, loc], csend.at[1], crecv.at[1],
            dev(1, 0, 0),
        ),
    ]
    moving = launch(0, V0, ZV.at[0], 0)

    for copy in coefs:
        copy.wait_recv()
    C[0, 1 : X + 1, PAD - 1, :] = YR[5, 0, 1]
    C[2, 1 : X + 1, PAD - 1, :] = YR[5, 0, 2]

    @pl.loop(0, X, unroll=UNROLL)
    def _(i):
        p = i + 1
        c0, c1, c2 = (C[c, p, loc, :] for c in range(3))
        c0z, c1z = dn_z(c0, CZ[0, i]), dn_z(c1, CZ[1, i])
        low = pl.ds(PAD - 1, Y)
        m0, m1, m2 = (m_ref[c, i] for c in range(3))
        E[0, p, loc, :] = 1.0 / (m0 + c1 + c1z + c2 + C[2, p, low, :])
        E[1, p, loc, :] = 1.0 / (m1 + c2 + C[2, i, loc, :] + c0 + c0z)
        E[2, p, loc, :] = 1.0 / (m2 + c0 + C[0, p, low, :] + c1 + C[1, i, loc, :])
        before = jnp.where(i == 0, MX[...], m_ref[0, jnp.maximum(i - 1, 0)])
        back = YR[5, 0, 0, pl.ds(i, 1), :]
        m1y = jnp.where(row == 0, jnp.broadcast_to(back, (Y, Z)), pltpu.roll(m1, 1, 0))
        E[3, p, loc, :] = 1.0 / (m0 + before + m1 + m1y + m2 + dn_z(m2, MZ[i]))

    stage(1, E, folded)
    e_moving = launch(1, E, ZE, 1)
    land(0, V0, ZV.at[0], straight, moving)
    land(1, E, ZE, folded, e_moving[:-2])

    line_lane = lax.broadcasted_iota(jnp.int32, (1, Z), 1)

    def share(k, n, slot):
        a, b, c = others[n]
        return pltpu.make_async_remote_copy(
            src_ref=RED.at[k, slot], dst_ref=RED.at[k, slot], send_sem=rsend.at[k, n],
            recv_sem=rrecv.at[k, slot], device_id=(xs[a], ys[b], zs[c]), device_id_type=MESH,
        )

    def start_sums(k, gamma, delta):
        packed = jnp.zeros((1, Z), jnp.float32)
        for n, value in enumerate((gamma, delta)):
            part = jnp.sum(jnp.sum(value, axis=0, keepdims=True), axis=1, keepdims=True)
            packed = jnp.where(line_lane == n, part, packed)
        RED[k, rank] = packed
        for n in range(len(others)):
            share(k, n, rank).start()

    def finish_sums(k):
        for n, (a, b, c) in enumerate(others):
            share(k, n, (xs[a] * ny + ys[b]) * nz + zs[c]).wait_recv()
        rows = [RED[k, n] for n in range(total)]
        while len(rows) > 1:
            rows = [sum(rows[n + 1 : n + 2], rows[n]) for n in range(0, len(rows), 2)]
        return [
            jnp.sum(jnp.where(line_lane == n, rows[0], 0.0), axis=1, keepdims=True)
            for n in range(2)
        ]

    gamma_old = alpha_old = None

    def step(k):
        gamma, delta = finish_sums(k)
        if k == 0:
            return gamma, gamma / delta, None
        beta = gamma / gamma_old
        return gamma, gamma / (delta - beta * gamma / alpha_old), beta

    full = pl.ds(0, Yh)
    full_up = pl.ds(1, Yh)
    low = pl.ds(PAD - 1, Y)
    high = pl.ds(PAD + 1, Y)
    hi_full = pl.ds(PAD, Yh)

    def fold(values):
        return jnp.sum(values.reshape(Y // 8, 8, Z), axis=0)

    for k in range(ITERS):
        W, ZW = V.at[k], ZV.at[k]
        if k:
            land(k + 1, W, ZW, straight, moving[:-2])

        def scaled(p, _):
            for c in range(3):
                S[c, p] = W[c, p] * E[c, p]
            return 0

        lax.fori_loop(1, X + 1, scaled, 0, unroll=UNROLL)

        def nodal(p, _):
            r2 = W[2, p, hi_full, :]
            q = (
                (W[0, p - 1, hi_full, :] - W[0, p, hi_full, :])
                + (W[1, p, pl.ds(PAD - 1, Yh), :] - W[1, p, hi_full, :])
                + (dn_z(r2, ZW[0, 2, p, hi_full, :]) - r2)
            )
            PH[p] = q * E[3, p, hi_full, :]
            return 0

        lax.fori_loop(2, X + 1, nodal, 0, unroll=UNROLL)

        def sz(side, c, p, rows):
            return ZW[side, c, p, rows, :] * ZE[side, c, p, rows, :]

        def curl_faces(p):
            s0, s1, s2 = (S[c, p, full, :] for c in range(3))
            g2 = C[2, p, full, :] * ((S[1, p + 1, full, :] - s1) - (S[0, p, full_up, :] - s0))
            t0, t2 = S[0, p, loc, :], S[2, p, loc, :]
            g1 = C[1, p, loc, :] * (
                (up_z(t0, sz(north, 0, p, loc)) - t0) - (S[2, p + 1, loc, :] - t2)
            )
            G[1, p, loc, :] = g1
            G[2, p, full, :] = g2
            return s1, s2

        def faces(p, _):
            s1, s2 = curl_faces(p)
            G[0, p, full, :] = C[0, p, full, :] * (
                (S[2, p, full_up, :] - s2) - (up_z(s1, sz(north, 1, p, full)) - s1)
            )
            return 0

        lax.fori_loop(1, X, faces, 0, unroll=UNROLL)

        for copy in (moving if k else e_moving)[-2:]:
            copy.wait_recv()
        for p in (0, X + 1):
            scaled(p, 0)
        for p in (1, X + 1):
            nodal(p, 0)
        curl_faces(0)
        faces(X, 0)

        if k:
            gamma_old, alpha_old, beta = step(k - 1)
            alpha = jnp.broadcast_to(alpha_old, (Y, Z))
            if k > 1:
                beta = jnp.broadcast_to(beta, (Y, Z))

        def apply(p, acc):
            i = p - 1
            s0, s1, s2 = (S[c, p, loc, :] for c in range(3))
            z0, z1, z2 = (sz(0, c, p, loc) for c in range(3))
            g0z = CZ[0, i] * ((sz(0, 2, p, high) - z2) - (pltpu.roll(s1, Z - 1, 1) - z1))
            g1z = CZ[1, i] * ((pltpu.roll(s0, Z - 1, 1) - z0) - (sz(0, 2, p + 1, loc) - z2))
            g0, g1, g2 = (G[c, p, loc, :] for c in range(3))
            g0b, g1b = dn_z(g0, g0z), dn_z(g1, g1z)
            n0 = ZW[north, 0, p, loc, :]
            n1 = ZW[north, 1, p, loc, :]
            qz = (
                (ZW[north, 0, i, loc, :] - n0)
                + (ZW[north, 1, p, low, :] - n1)
                + (pltpu.roll(W[2, p, loc, :], 1, 1) - ZW[north, 2, p, loc, :])
            )
            here = PH[p, 0:Y, :]
            b0 = s0 + (PH[p + 1, 0:Y, :] - here)
            b1 = s1 + (PH[p, 1 : Y + 1, :] - here)
            b2 = s2 + (up_z(here, qz * ZE[north, 3, p, loc, :]) - here)
            b = (b0, b1, b2)
            a = (
                (g1b - g1) - (G[2, p, low, :] - g2),
                (G[2, i, loc, :] - g2) - (g0b - g0),
                (G[0, p, low, :] - g0) - (G[1, i, loc, :] - g1),
            )
            w = [W[c, p, loc, :] for c in range(3)]
            gamma, delta = acc
            terms = [[], []]
            for c in range(3):
                n = a[c] + m_ref[c, i] * b[c]
                if k == 0:
                    res, pre, img = w[c], b[c], n
                else:
                    u = ST[0, c, i]
                    prev = V[0, c, p, loc, :] if k == 1 else ST[6, c, i]
                    zz, qq, ss, pp = n, b[c], w[c], u
                    if k > 1:
                        zz = zz + beta * ST[1, c, i]
                        qq = qq + beta * ST[2, c, i]
                        ss = ss + beta * ST[3, c, i]
                        pp = pp + beta * ST[4, c, i]
                    if k + 1 < ITERS:
                        ST[1, c, i] = zz
                        ST[2, c, i] = qq
                    ST[3, c, i] = ss
                    ST[4, c, i] = pp
                    ST[5, c, i] = alpha * pp if k == 1 else ST[5, c, i] + alpha * pp
                    res, pre, img = prev - alpha * ss, u - alpha * qq, w[c] - alpha * zz
                    ST[6, c, i] = res
                ST[0, c, i] = pre
                if k + 1 < ITERS:
                    V[k + 1, c, p, loc, :] = img
                else:
                    WL[c, i] = img
                terms[0].append(res * pre)
                terms[1].append(img * pre)
            return (
                gamma + fold(terms[0][0] + terms[0][1] + terms[0][2]),
                delta + fold(terms[1][0] + terms[1][1] + terms[1][2]),
            )

        zero = jnp.zeros((8, Z), jnp.float32)
        gamma, delta = lax.fori_loop(1, X + 1, apply, (zero, zero), unroll=UNROLL)
        if k + 1 < ITERS:
            stage(k + 2, V.at[k + 1], straight)
            moving = launch(
                k + 2, V.at[k + 1], ZV.at[k + 1], 0, lambda: start_sums(k, gamma, delta)
            )
        else:
            start_sums(k, gamma, delta)

    _, alpha, beta = step(ITERS - 1)
    alpha = jnp.broadcast_to(alpha, (Y, Z))
    beta = jnp.broadcast_to(beta, (Y, Z))

    @pl.loop(0, X, unroll=UNROLL)
    def _(i):
        for c in range(3):
            x_out[c, i] = ST[5, c, i] + alpha * (ST[0, c, i] + beta * ST[4, c, i])
            res_out[c, i] = ST[6, c, i] - alpha * (WL[c, i] + beta * ST[3, c, i])

    for copy in pending:
        copy.wait_send()
    for k in range(ITERS):
        for n in range(len(others)):
            share(k, n, rank).wait_send()


def body(sizes, right_side, mass_coef, curl_coef):
    _, X, Y, Z = right_side.shape
    nx, ny, nz = sizes
    total = nx * ny * nz
    sides = 1 if nz == 2 else 2
    XE, YE, Yh = X + 2, Y + 2 * PAD, Y + PAD
    f32 = jnp.float32
    vmem = pl.BlockSpec(memory_space=pltpu.VMEM)
    phases = ITERS + 1
    dma = pltpu.SemaphoreType.DMA
    return pl.pallas_call(
        functools.partial(kernel, sizes),
        out_shape=[jax.ShapeDtypeStruct(right_side.shape, f32)] * 2,
        in_specs=[pl.BlockSpec(memory_space=pltpu.HBM)] * 3,
        out_specs=[vmem] * 2,
        scratch_shapes=[
            pltpu.VMEM((ITERS, 3, XE, YE, Z), f32),
            pltpu.VMEM((4, XE, YE, Z), f32),
            pltpu.VMEM((3, XE, YE, Z), f32),
            pltpu.VMEM((ITERS, sides, 3, XE, YE, Z), f32),
            pltpu.VMEM((sides, 4, XE, YE, Z), f32),
            pltpu.VMEM((2, X, Y, Z), f32),
            pltpu.VMEM((Y, Z), f32),
            pltpu.VMEM((X, Y, Z), f32),
            pltpu.VMEM((phases + 1, 2, 3, X, Z), f32),
            pltpu.VMEM((phases + 1, 2, 3, X, Z), f32),
            pltpu.VMEM((phases, 6, 1, Z), f32),
            pltpu.VMEM((phases, 6, 1, Z), f32),
            pltpu.VMEM((XE, Yh, Z), f32),
            pltpu.VMEM((3, XE, YE, Z), f32),
            pltpu.VMEM((3, XE, YE, Z), f32),
            pltpu.VMEM((7, 3, X, Y, Z), f32),
            pltpu.VMEM((3, X, Y, Z), f32),
            pltpu.VMEM((ITERS, total, 1, Z), f32),
            dma((phases, 10 + sides)),
            dma((phases, 10 + sides)),
            dma((5,)),
            dma((5,)),
            dma((ITERS, total)),
            dma((ITERS, total)),
            pltpu.VMEM((3, X, Y, Z), f32),
            dma((3,)),
        ],
        compiler_params=pltpu.CompilerParams(
            collective_id=0, has_side_effects=True, vmem_limit_bytes=24 * 1024 * 1024
        ),
        name="relayed_cg",
    )(*(pltpu.with_memory_space_constraint(a, pltpu.HBM) for a in (right_side, mass_coef, curl_coef)))


def solution(mesh):
    sizes = tuple(mesh.shape[a] for a in ("gx", "gy", "gz"))
    spec = P(None, "gx", "gy", "gz")
    return jax.shard_map(
        functools.partial(body, sizes), mesh=mesh, in_specs=(spec,) * 3, out_specs=(spec, spec),
        check_vma=False,
    )
```
